32 devices in a mesh: replica: 1 (over z), data: 32 (over y, x, core).
Axes of the slice: x: 4, y: 4, z: 1, core: 2. Of those that a mesh axis runs over, the one named last changes fastest.
The devices are a block of a 4x4x8 slice.
Arguments:
- x: bfloat16 [8192, 2048], P(('replica', 'data'))
- adapter_id: int32 [8192], P(('replica', 'data'))
- w_gate: bfloat16 [2048, 11008], replicated
- w_up: bfloat16 [2048, 11008], replicated
- w_down: bfloat16 [11008, 2048], replicated
- a_gate: bfloat16 [64, 2048, 32], P('data')
- b_gate: bfloat16 [64, 32, 11008], P('data')
- a_up: bfloat16 [64, 2048, 32], P('data')
- b_up: bfloat16 [64, 32, 11008], P('data')
- a_down: bfloat16 [64, 11008, 32], P('data')
- b_down: bfloat16 [64, 32, 2048], P('data')
- hot_ids: int32 [4], replicated
- hot_a_gate: bfloat16 [4, 2048, 32], replicated
- hot_b_gate: bfloat16 [4, 32, 11008], replicated
- hot_a_up: bfloat16 [4, 2048, 32], replicated
- hot_b_up: bfloat16 [4, 32, 11008], replicated
- hot_a_down: bfloat16 [4, 11008, 32], replicated
- hot_b_down: bfloat16 [4, 32, 2048], replicated
Outputs:
- output: bfloat16 [8192, 2048], P(('replica', 'data'))
All inputs are finite; a program needn't handle non-finite values.
Results may differ from the reference program's by a relative error of at most 0.00644598.
Values are sent between devices in bfloat16 or wider.
A program may use at most 768 MiB of HBM per device.

```python
import jax
import jax.numpy as jnp
from jax import lax

GROUP = 32
T_LOC = 256
D = 2048
F = 11008
R = 32
N_LOC = 2
HOT_K = 4
LORA_ALPHA = 32
TOK_BLOCK = 128
TOKENS = GROUP * T_LOC
ADAPTERS = GROUP * N_LOC
CAP = T_LOC // (2 * GROUP)
LORA_SCALE = LORA_ALPHA / R


def draw_hot(hot_key):
    owner_key, local_key = jax.random.split(hot_key)
    hot_owner = jax.random.permutation(owner_key, GROUP)[:HOT_K]
    hot_local = jax.random.randint(local_key, (HOT_K,), 0, N_LOC)
    return hot_owner, hot_local


def draw_ids(id_key, hot_owner, hot_local):
    shift_key, peak_key, count_key, perm_key, cold_key, pick_key = jax.random.split(id_key, 6)
    owners = jnp.arange(GROUP)
    peak_owner = jax.random.randint(peak_key, (), 0, GROUP)
    pop_shift = jnp.where(owners == peak_owner, 0, jax.random.randint(shift_key, (GROUP,), 0, 4))
    cap_upper = jnp.maximum(CAP // (2 ** pop_shift), 1)
    cap_lower = jnp.maximum(cap_upper // 2, 1)
    counts = jax.random.randint(count_key, (GROUP, GROUP), cap_lower[None, :], cap_upper[None, :] + 1)
    counts = jnp.where(owners[None, :] == peak_owner, CAP, counts)
    count_ends = jnp.cumsum(counts, axis=1)
    positions = jnp.arange(T_LOC)

    def owner_row(end_row):
        return jnp.searchsorted(end_row, positions, side='right')

    owner_seq = jax.vmap(owner_row)(count_ends)
    owner_seq = jax.random.permutation(perm_key, owner_seq, axis=1, independent=True)
    owner_safe = jnp.minimum(owner_seq, GROUP - 1)
    hot_match = hot_owner[None, :] == owners[:, None]
    has_hot = jnp.any(hot_match, axis=1).astype(jnp.int32)
    skip_local = jnp.sum(jnp.where(hot_match, hot_local[None, :], 0), axis=1) + (1 - has_hot) * N_LOC
    pick_local = jax.random.randint(cold_key, (GROUP, T_LOC), 0, N_LOC - has_hot[owner_safe])
    pick_local = pick_local + (pick_local >= skip_local[owner_safe]).astype(jnp.int32)
    cold_ids = owner_safe * N_LOC + pick_local
    hot_list = hot_owner * N_LOC + hot_local
    hot_tok = hot_list[jax.random.randint(pick_key, (GROUP, T_LOC), 0, HOT_K)]
    tok_ids = jnp.where(owner_seq == GROUP, hot_tok, cold_ids)
    return tok_ids.reshape(TOKENS).astype(jnp.int32)


def normal_weights(w_key, shape, std):
    return (jax.random.normal(w_key, shape, jnp.float32) * std).astype(jnp.bfloat16)


def adapter_set(set_key, adapter_count):
    set_keys = jax.random.split(set_key, 6)
    b_std = 0.5 / (LORA_SCALE * R ** 0.5)
    return [
        normal_weights(set_keys[0], (adapter_count, D, R), D ** -0.5),
        normal_weights(set_keys[1], (adapter_count, R, F), b_std),
        normal_weights(set_keys[2], (adapter_count, D, R), D ** -0.5),
        normal_weights(set_keys[3], (adapter_count, R, F), b_std),
        normal_weights(set_keys[4], (adapter_count, F, R), F ** -0.5),
        normal_weights(set_keys[5], (adapter_count, R, D), b_std),
    ]


def setup_inputs(seed: int = 0, part: int = 0) -> dict:
    root_key = jax.random.key(seed)
    base_keys = jax.random.split(jax.random.fold_in(root_key, 1), 3)
    route_key = jax.random.fold_in(root_key, 3)
    hot_owner, hot_local = draw_hot(jax.random.fold_in(route_key, 2))
    tok_ids = draw_ids(jax.random.fold_in(jax.random.fold_in(route_key, 1), part), hot_owner, hot_local)
    x_key = jax.random.fold_in(jax.random.fold_in(root_key, 5), part)
    store_set = adapter_set(jax.random.fold_in(root_key, 2), ADAPTERS)
    hot_set = adapter_set(jax.random.fold_in(root_key, 4), HOT_K)
    return {
        'x': jax.random.normal(x_key, (TOKENS, D), jnp.float32).astype(jnp.bfloat16),
        'adapter_id': tok_ids,
        'w_gate': normal_weights(base_keys[0], (D, F), D ** -0.5),
        'w_up': normal_weights(base_keys[1], (D, F), D ** -0.5),
        'w_down': normal_weights(base_keys[2], (F, D), F ** -0.5),
        'a_gate': store_set[0],
        'b_gate': store_set[1],
        'a_up': store_set[2],
        'b_up': store_set[3],
        'a_down': store_set[4],
        'b_down': store_set[5],
        'hot_ids': (hot_owner * N_LOC + hot_local).astype(jnp.int32),
        'hot_a_gate': hot_set[0],
        'hot_b_gate': hot_set[1],
        'hot_a_up': hot_set[2],
        'hot_b_up': hot_set[3],
        'hot_a_down': hot_set[4],
        'hot_b_down': hot_set[5],
    }


def lora_delta(tok_rows, a_rows, b_rows):
    low_rank = jnp.einsum('td,tdr->tr', tok_rows.astype(jnp.float32), a_rows.astype(jnp.float32)).astype(jnp.bfloat16)
    delta_f = jnp.einsum('tr,trf->tf', low_rank.astype(jnp.float32), b_rows.astype(jnp.float32))
    return (LORA_SCALE * delta_f).astype(jnp.bfloat16)


def reference(x, adapter_id, w_gate, w_up, w_down, a_gate, b_gate, a_up, b_up, a_down, b_down, hot_ids, hot_a_gate, hot_b_gate, hot_a_up, hot_b_up, hot_a_down, hot_b_down):
    def block_out(block_args):
        tok_rows, tok_ids = block_args
        hot_match = tok_ids[:, None] == hot_ids[None, :]
        is_hot = jnp.any(hot_match, axis=1)
        hot_slot = jnp.sum(jnp.where(hot_match, jnp.arange(HOT_K)[None, :], 0), axis=1)

        def chosen(store_set, hot_copy):
            return jnp.where(is_hot[:, None, None], hot_copy[hot_slot], store_set[tok_ids])

        gate_act = jnp.dot(tok_rows, w_gate, preferred_element_type=jnp.float32) + lora_delta(tok_rows, chosen(a_gate, hot_a_gate), chosen(b_gate, hot_b_gate)).astype(jnp.float32)
        up_act = jnp.dot(tok_rows, w_up, preferred_element_type=jnp.float32) + lora_delta(tok_rows, chosen(a_up, hot_a_up), chosen(b_up, hot_b_up)).astype(jnp.float32)
        hidden = (jax.nn.silu(gate_act) * up_act).astype(jnp.bfloat16)
        down_out = jnp.dot(hidden, w_down, preferred_element_type=jnp.float32) + lora_delta(hidden, chosen(a_down, hot_a_down), chosen(b_down, hot_b_down)).astype(jnp.float32)
        return (tok_rows.astype(jnp.float32) + down_out).astype(jnp.bfloat16)

    blocks = lax.map(block_out, (x.reshape(TOKENS // TOK_BLOCK, TOK_BLOCK, D), adapter_id.reshape(TOKENS // TOK_BLOCK, TOK_BLOCK)))
    return blocks.reshape(TOKENS, D)
```

```python
import functools

import jax
import jax.numpy as jnp
from jax import lax
from jax.experimental import pallas as pl
from jax.experimental.pallas import tpu as pltpu
from jax.sharding import PartitionSpec as P

value_a10 = 32
MESH = pl.DeviceIdType.MESH
F32 = jnp.float32
BF16 = jnp.bfloat16
ROWS = 16
TILE = 512
SLOTS = 7
LANES = 128


def dot(a, b):
    return jnp.dot(a, b, preferred_element_type=F32)


def dot_nt(a, b):
    return lax.dot_general(a, b, (((1,), (1,)), ((), ())), preferred_element_type=F32)


def iota(shape, dim):
    return lax.broadcasted_iota(jnp.int32, shape, dim)


def mlp_kernel(cfg, ids_ref, hot_ref, x_hbm, wg, wu, wd, ag, bg, au, bu, ad, bd, hag, hbg, hau, hbu, had, hbd, out_hbm,
               x_v, xp_v, pt_v, fold_v, unfold_v, send_v, recv_v, h_v, ring, ag_v, au_v, bg_v, bu_v, ad_v, bd_v,
               lrg_v, lru_v, mask_v, accl_v, ret_v, back_v, yl_v, out_v,
               w_sem, l_sem, x_sem, send_sem, recv_sem, rsend_sem, rrecv_sem, out_sem):
    G, T, D, F, CAP, NL, RK, HK = cfg["G"], cfg["T"], cfg["D"], cfg["F"], cfg["CAP"], cfg["NL"], cfg["RK"], cfg["HK"]
    scale = cfg["scale"]
    Q = ROWS // CAP
    R = G * CAP
    CQ = D // Q
    SR = G * ROWS
    HOT = HK * RK
    LR = HOT + NL * RK
    me = lax.axis_index("data")
    shift = CAP.bit_length() - 1
    rshift = ROWS.bit_length() - 1

    NA = -(-F // TILE)
    tail = F - (NA - 1) * TILE
    NB = D // TILE
    WR = 2 * D
    NP = -(-F // WR)
    ptail = F - (NP - 1) * WR
    NC = NA + NB * NP

    def up_copies(c, width):
        slot = lax.rem(c, SLOTS)
        col = pl.ds(pl.multiple_of(c * TILE, TILE), width)
        return [pltpu.make_async_copy(w.at[:, col], ring.at[slot, pl.ds(k * D, D), pl.ds(0, width)], w_sem.at[slot, k])
                for k, w in enumerate((wg, wu))]

    def down_copy(c, rows):
        slot = lax.rem(c, SLOTS)
        i = c - NA
        blk, part = i // NP, lax.rem(i, NP)
        row = pl.ds(pl.multiple_of(part * WR, 16), rows)
        col = pl.ds(pl.multiple_of(blk * TILE, TILE), TILE)
        return pltpu.make_async_copy(wd.at[row, col], ring.at[slot, pl.ds(0, rows), :], w_sem.at[slot, 0])

    def start_chunk(c):
        @pl.when(c < NA - 1)
        def _():
            for cp in up_copies(c, TILE):
                cp.start()

        @pl.when(c == NA - 1)
        def _():
            for cp in up_copies(NA - 1, tail):
                cp.start()

        @pl.when(jnp.logical_and(c >= NA, c < NC))
        def _():
            part = lax.rem(c - NA, NP)

            @pl.when(part < NP - 1)
            def _():
                down_copy(c, WR).start()

            @pl.when(part == NP - 1)
            def _():
                down_copy(c, ptail).start()

    x_copy = pltpu.make_async_copy(x_hbm, x_v, x_sem)
    x_copy.start()
    lora = []
    for i, (hot_w, own_w, buf) in enumerate(((hag, ag, ag_v), (hau, au, au_v), (hbg, bg, bg_v), (hbu, bu, bu_v), (had, ad, ad_v), (hbd, bd, bd_v))):
        lora.append((pltpu.make_async_copy(hot_w, buf.at[pl.ds(0, HOT), :], l_sem.at[i, 0]),
                     pltpu.make_async_copy(own_w, buf.at[pl.ds(HOT, NL * RK), :], l_sem.at[i, 1])))
    for pair in lora:
        for cp in pair:
            cp.start()
    for c in range(min(SLOTS, NC)):
        start_chunk(jnp.int32(c))

    barrier = pltpu.get_barrier_semaphore()

    @pl.loop(1, G)
    def _(k):
        pl.semaphore_signal(barrier, inc=1, device_id={"data": lax.rem(me + k, G)}, device_id_type=MESH)

    ids = ids_ref[...]
    hotf = jnp.zeros((1, T), F32)
    for j in range(HK):
        hotf = jnp.where(ids == hot_ref[j], 1.0, hotf)
    lo = iota((G, T), 0) * NL
    own = jnp.where(jnp.logical_and(ids >= lo, ids < lo + NL), 1.0 - hotf, 0.0)
    before = jnp.where(iota((T, T), 0) < iota((T, T), 1), 1.0, 0.0).astype(BF16)
    rank = dot(own.astype(BF16), before)
    hot_rank = dot(jnp.broadcast_to(hotf, (16, T)).astype(BF16), before)[0:1, :]
    slot_own = jnp.where((iota((R, G), 0) >> shift) == iota((R, G), 1), 1.0, 0.0).astype(BF16)
    own_s = dot(slot_own, own.astype(BF16))
    rank_s = dot(slot_own, rank.astype(BF16))
    place = (iota((R, T), 0) & (CAP - 1)).astype(F32)
    cold = jnp.where(rank_s == place, own_s, 0.0)
    free = 1.0 - jnp.sum(cold, axis=1, keepdims=True)
    earlier = jnp.where(iota((R, R), 1) < iota((R, R), 0), 1.0, 0.0).astype(BF16)
    free_rank = dot(earlier, jnp.broadcast_to(free, (R, LANES)).astype(BF16))[:, 0:1]
    fill = jnp.where(free_rank == hot_rank, free * hotf, 0.0)
    n_free = jnp.sum(free, axis=0, keepdims=True)
    keep = jnp.where(hot_rank - n_free == iota((R, T), 0).astype(F32), hotf, 0.0)
    perm = jnp.concatenate([cold + fill, keep], axis=0)
    pt_v[...] = jnp.transpose(perm).astype(BF16)
    slot_id = jnp.sum(perm * ids.astype(F32), axis=1, keepdims=True)
    slot_id = jnp.broadcast_to(slot_id, (T, LANES))
    perm = perm.astype(BF16)

    def fold_of(row, col):
        owner, grp, c = row >> rshift, (row & (ROWS - 1)) >> shift, row & (CAP - 1)
        return jnp.where(grp * R + owner * CAP + c == col, 1.0, 0.0).astype(BF16)

    fold_v[...] = fold_of(iota((SR, SR), 0), iota((SR, SR), 1))
    unfold_v[...] = fold_of(iota((SR, SR), 1), iota((SR, SR), 0))

    x_copy.wait()
    stack = []
    for q in range(Q):
        part = dot(perm, x_v[:, q * CQ:(q + 1) * CQ]).astype(BF16)
        stack.append(part[:R])
        xp_v[R:, q * CQ:(q + 1) * CQ] = part[R:]
    send_v[:, :CQ] = dot(fold_v[...], jnp.concatenate(stack, axis=0)).astype(BF16)
    send_v[:, CQ:] = dot(fold_v[...], jnp.concatenate([slot_id[:R]] * Q, axis=0).astype(BF16)).astype(BF16)
    mine = pl.ds(pl.multiple_of(me * ROWS, ROWS), ROWS)
    recv_v[mine, :] = send_v[mine, :]

    pl.semaphore_wait(barrier, G - 1)

    def send_copy(k):
        peer = lax.rem(me + k, G)
        return pltpu.make_async_remote_copy(
            src_ref=send_v.at[pl.ds(pl.multiple_of(peer * ROWS, ROWS), ROWS), :], dst_ref=recv_v.at[mine, :],
            send_sem=send_sem, recv_sem=recv_sem, device_id={"data": peer}, device_id_type=MESH)

    @pl.loop(1, G)
    def _(k):
        send_copy(k).start()

    bulk = pl.ds(0, (G - 1) * ROWS)
    all_sends = pltpu.make_async_remote_copy(
        src_ref=send_v.at[bulk, :], dst_ref=recv_v.at[bulk, :], send_sem=send_sem, recv_sem=recv_sem,
        device_id={"data": me}, device_id_type=MESH)
    all_sends.wait_recv()

    got = dot(unfold_v[...], recv_v[:, :CQ]).astype(BF16)
    for q in range(Q):
        xp_v[:R, q * CQ:(q + 1) * CQ] = got[q * R:(q + 1) * R]
    got_id = dot(unfold_v[:R, :], recv_v[:, CQ:])
    row_id = jnp.concatenate([got_id, slot_id[R:]], axis=0)

    lane = iota((1, HOT), 1)
    hot_lane = jnp.zeros((1, HOT), F32)
    is_hot = jnp.zeros((T, LANES), F32)
    for j in range(HK):
        hid = hot_ref[j].astype(F32)
        hot_lane = jnp.where(lane // RK == j, hid, hot_lane)
        is_hot = jnp.where(row_id == hid, 1.0, is_hot)
    own_lane = (me * NL + iota((1, NL * RK), 1) // RK).astype(F32)
    hot_mask = jnp.where(row_id[:, :HOT] == hot_lane, 1.0, 0.0)
    own_mask = jnp.where(row_id[:, :NL * RK] == own_lane, 1.0 - is_hot[:, :NL * RK], 0.0)
    mask_v[...] = jnp.concatenate([hot_mask, own_mask], axis=1)

    def low_rank(acc):
        return jnp.where(mask_v[...] > 0.5, acc, 0.0).astype(BF16)

    def delta(low, b):
        d = dot(low, b)
        if scale != 1.0:
            d = scale * d
        return d.astype(BF16).astype(F32)

    for pair in lora:
        for cp in pair:
            cp.wait()
    lrg_v[...] = low_rank(dot_nt(xp_v[...], ag_v[...]))
    lru_v[...] = low_rank(dot_nt(xp_v[...], au_v[...]))
    accl_v[...] = jnp.zeros((T, LR), F32)

    def up_chunk(c, width):
        slot = lax.rem(c, SLOTS)
        col = pl.ds(pl.multiple_of(c * TILE, TILE), width)
        for cp in up_copies(c, width):
            cp.wait()
        g = dot(xp_v[...], ring[slot, :D, :width]) + delta(lrg_v[...], bg_v[:, col])
        u = dot(xp_v[...], ring[slot, D:2 * D, :width]) + delta(lru_v[...], bu_v[:, col])
        h = (jax.nn.silu(g) * u).astype(BF16)
        h_v[:, col] = h
        accl_v[...] += dot_nt(h, ad_v[:, col])
        start_chunk(jnp.int32(c + SLOTS))

    @pl.loop(0, NA - 1)
    def _(c):
        up_chunk(c, TILE)

    up_chunk(jnp.int32(NA - 1), tail)
    lrd = low_rank(accl_v[...])
    lrg_v[...] = lrd

    def ret_copy(b, k):
        peer = lax.rem(me + k, G)
        return pltpu.make_async_remote_copy(
            src_ref=ret_v.at[b, pl.ds(pl.multiple_of(peer * ROWS, ROWS), ROWS), :], dst_ref=back_v.at[b, mine, :],
            send_sem=rsend_sem.at[b], recv_sem=rrecv_sem.at[b], device_id={"data": peer}, device_id_type=MESH)

    def ret_all(b):
        return pltpu.make_async_remote_copy(
            src_ref=ret_v.at[b, bulk, :], dst_ref=back_v.at[b, bulk, :],
            send_sem=rsend_sem.at[b], recv_sem=rrecv_sem.at[b], device_id={"data": me}, device_id_type=MESH)

    TQ = TILE // Q

    @pl.loop(0, NB)
    def _(b):
        acc = jnp.zeros((T, TILE), F32)
        for part in range(NP):
            rows = WR if part < NP - 1 else ptail
            c = NA + b * NP + part
            slot = lax.rem(c, SLOTS)
            down_copy(c, rows).wait()
            acc += dot(h_v[:, part * WR:part * WR + rows], ring[slot, :rows, :])
            start_chunk(jnp.int32(c + SLOTS))
        col = pl.ds(pl.multiple_of(b * TILE, TILE), TILE)
        y = acc + delta(lrg_v[...], bd_v[:, col])
        o = (xp_v[:, col].astype(F32) + y).astype(BF16)
        yl_v[:, col] = o[R:]
        folded = dot(fold_v[...], jnp.concatenate([o[:R, q * TQ:(q + 1) * TQ] for q in range(Q)], axis=0))
        ret_v[b] = folded.astype(BF16)
        back_v[b, mine, :] = ret_v[b, mine, :]

        @pl.loop(1, G)
        def _(k):
            ret_copy(b, k).start()

    all_sends.wait_send()

    def out_copy(b):
        col = pl.ds(pl.multiple_of(b * TILE, TILE), TILE)
        return pltpu.make_async_copy(out_v.at[:, col], out_hbm.at[:, col], out_sem.at[b])

    @pl.loop(0, NB)
    def _(b):
        col = pl.ds(pl.multiple_of(b * TILE, TILE), TILE)
        ret_all(b).wait_recv()
        flat = dot(unfold_v[...], back_v[b]).astype(BF16)
        top = jnp.concatenate([flat[q * R:(q + 1) * R] for q in range(Q)], axis=1)
        y = jnp.concatenate([top, yl_v[:, col]], axis=0)
        out_v[:, col] = dot(pt_v[...], y).astype(BF16)
        out_copy(b).start()

    @pl.loop(0, NB)
    def _(b):
        ret_all(b).wait_send()
        out_copy(b).wait()


def solution(mesh):
    group_size = mesh.shape["data"]
    token_spec = P(("replica", "data"), None)
    store_spec = P("data", None, None)
    full_mat = P(None, None)
    full_set = P(None, None, None)
    in_specs = (token_spec, P(("replica", "data")), full_mat, full_mat, full_mat) + (store_spec,) * 6 + (P(None),) + (full_set,) * 6

    def device_step(x, adapter_id, w_gate, w_up, w_down, a_gate, b_gate, a_up, b_up, a_down, b_down, hot_ids, hot_a_gate, hot_b_gate, hot_a_up, hot_b_up, hot_a_down, hot_b_down):
        T, D = x.shape
        F = w_gate.shape[1]
        NL, _, RK = a_gate.shape
        HK = hot_ids.shape[0]
        G = group_size
        CAP = T // (2 * G)
        Q = ROWS // CAP
        R = G * CAP
        LR = (HK + NL) * RK
        SR = G * ROWS
        NB = D // TILE
        assert CAP & (CAP - 1) == 0 and D % (Q * LANES) == 0 and G * NL <= 256
        cfg = dict(G=G, T=T, D=D, F=F, CAP=CAP, NL=NL, RK=RK, HK=HK, scale=value_a10 / RK)

        def a_rows(a):
            return jnp.swapaxes(a, 1, 2).reshape(-1, a.shape[1])

        def b_rows(b):
            return b.reshape(-1, b.shape[2])

        hbm = pl.BlockSpec(memory_space=pl.ANY)
        vmem = pl.BlockSpec(memory_space=pltpu.VMEM)
        smem = pl.BlockSpec(memory_space=pltpu.SMEM)
        dma = pltpu.SemaphoreType.DMA
        scratch = [
            pltpu.VMEM((T, D), BF16), pltpu.VMEM((T, D), BF16), pltpu.VMEM((T, T), BF16),
            pltpu.VMEM((SR, SR), BF16), pltpu.VMEM((SR, SR), BF16),
            pltpu.VMEM((SR, D // Q + LANES), BF16), pltpu.VMEM((SR, D // Q + LANES), BF16),
            pltpu.VMEM((T, F), BF16), pltpu.VMEM((SLOTS, 2 * D, TILE), BF16),
            pltpu.VMEM((LR, D), BF16), pltpu.VMEM((LR, D), BF16), pltpu.VMEM((LR, F), BF16), pltpu.VMEM((LR, F), BF16),
            pltpu.VMEM((LR, F), BF16), pltpu.VMEM((LR, D), BF16),
            pltpu.VMEM((T, LR), BF16), pltpu.VMEM((T, LR), BF16), pltpu.VMEM((T, LR), F32), pltpu.VMEM((T, LR), F32),
            pltpu.VMEM((NB, SR, TILE // Q), BF16), pltpu.VMEM((NB, SR, TILE // Q), BF16),
            pltpu.VMEM((R, D), BF16), pltpu.VMEM((T, D), BF16),
            dma((SLOTS, 2)), dma((6, 2)), dma, dma, dma, dma((NB,)), dma((NB,)), dma((NB,)),
        ]
        flops = 2 * T * (3 * D * F + LR * (3 * D + 3 * F))
        return pl.pallas_call(
            functools.partial(mlp_kernel, cfg),
            out_shape=jax.ShapeDtypeStruct((T, D), BF16),
            in_specs=[vmem, smem] + [hbm] * 16,
            out_specs=hbm,
            scratch_shapes=scratch,
            compiler_params=pltpu.CompilerParams(collective_id=0, has_side_effects=True, vmem_limit_bytes=67043328),
            cost_estimate=pl.CostEstimate(flops=flops, bytes_accessed=6 * D * F, transcendentals=T * F),
        )(adapter_id.reshape(1, T), hot_ids, x, w_gate, w_up, w_down,
          a_rows(a_gate), b_rows(b_gate), a_rows(a_up), b_rows(b_up), a_rows(a_down), b_rows(b_down),
          a_rows(hot_a_gate), b_rows(hot_b_gate), a_rows(hot_a_up), b_rows(hot_b_up), a_rows(hot_a_down), b_rows(hot_b_down))

    return jax.shard_map(device_step, mesh=mesh, in_specs=in_specs, out_specs=token_spec, check_vma=False)
```
